256 devices in a mesh: groups: 2 (over y), blk: 16 (over z), head: 4 (over x), rep: 2 (over core).
Axes of the slice: x: 4, y: 2, z: 16, core: 2. Of those that a mesh axis runs over, the one named last changes fastest.
The devices are a block of a 4x16x16 slice.
Arguments:
- queries: bfloat16 [8, 4096, 1024], P('groups', ('blk', 'rep'), 'head'), parts along dimension 0, may hold values from -24 to 24
- prefix_keys: bfloat16 [8, 8192, 128], P('groups', ('blk', 'head')), parts along dimension 0, may hold values from -6 to 6
- prefix_values: bfloat16 [8, 8192, 128], P('groups', ('blk', 'head')), parts along dimension 0, may hold values from -6 to 6
- stretch_keys: bfloat16 [8, 4096, 128], P('groups', ('blk', 'head')), parts along dimension 0, may hold values from -6 to 6
- stretch_values: bfloat16 [8, 4096, 128], P('groups', ('blk', 'head')), parts along dimension 0, may hold values from -6 to 6
- prefix_lengths: int32 [8], P('groups'), parts along dimension 0, may hold values from 128 to 8192, as said below
- decode_queries: bfloat16 [8, 64, 1024], P('groups', 'rep'), parts along dimension 0, may hold values from -24 to 24
- new_keys: bfloat16 [8, 64, 128], P('groups', 'rep'), parts along dimension 0, may hold values from -6 to 6
- new_values: bfloat16 [8, 64, 128], P('groups', 'rep'), parts along dimension 0, may hold values from -6 to 6
- row_prompts: int32 [128], P(('groups', 'rep')), parts along dimension 0, may hold values from 0 to 3
Outputs:
- prefill_out: bfloat16 [8, 4096, 1024], P('groups', ('blk', 'rep'), 'head'), parts along dimension 0
- decode_out: bfloat16 [8, 64, 1024], P('groups', 'rep'), parts along dimension 0
The draws below stay inside these ranges and needn't reach their ends.
There are 2 independent parts, one for each index of `groups`. The reference program is written for one: setup_inputs(seed, part) draws one part's arguments, and reference() takes and returns one part's arrays. A program takes and returns all parts, laid end to end along the dimension named above; each array names one. Nothing has to cross between parts.
Inputs may be any that keep to these rules, and one draw needn't show every extreme that they name: `prefix_lengths`: multiples of 128; in every draw some prompt has exactly 8192.
All inputs are finite; a program needn't handle non-finite values.
Results may differ from the reference program's by a relative error of at most 0.0095.
Values may be sent and summed in bfloat16 or wider, within the bound.
No kernel may reach another device: no remote copies, remote signals or barrier semaphores. Data moves between devices by JAX's collectives and lax.ppermute only.
A program may use at most 192 MiB of HBM per device.

```python
import jax
import jax.numpy as jnp
from jax import lax

HEADS = 8
HEAD_DIM = 128
PREFIX = 8192
STRETCH = 4096
STEPS = 4
ROWS = 64
PROMPTS = 4


def drawn_keys(key, salt, shape):
    subkey = jax.random.fold_in(key, salt)
    values = jnp.clip(jax.random.normal(subkey, shape, jnp.float32), -6.0, 6.0)
    return values.astype(jnp.bfloat16)


def drawn_queries(key, salt, shape):
    subkey = jax.random.fold_in(key, salt)
    values = jnp.clip(jax.random.normal(subkey, shape, jnp.float32), -6.0, 6.0)
    return values.astype(jnp.bfloat16)


def draw_queries(key, part):
    return drawn_queries(key, 11, (PROMPTS, STRETCH, HEADS * HEAD_DIM))


def draw_prefix_keys(key, part):
    return drawn_keys(key, 12, (PROMPTS, PREFIX, HEAD_DIM))


def draw_stretch_keys(key, part):
    return drawn_keys(key, 13, (PROMPTS, STRETCH, HEAD_DIM))


def draw_decode_queries(key, part):
    return drawn_queries(key, 14, (STEPS, ROWS, HEADS * HEAD_DIM))


def draw_new_keys(key, part):
    return drawn_keys(key, 15, (STEPS, ROWS, HEAD_DIM))


def draw_prefix_lengths(key, part):
    whole_units = PREFIX // 128
    units = jax.random.randint(jax.random.fold_in(key, 16), (PROMPTS,), 1, whole_units + 1)
    fullest = jax.random.randint(jax.random.fold_in(key, 17), (), 0, PROMPTS)
    units = jnp.where(jnp.arange(PROMPTS, dtype=jnp.int32) == fullest, whole_units, units)
    return (units * 128).astype(jnp.int32)


def plant(values, rng, low, high):
    shape = values.shape
    place = [jax.random.randint(jax.random.fold_in(rng, axis), (), 0, shape[axis]) for axis in range(len(shape))]
    values = values.at[tuple(place)].set(low)
    longest = shape.index(max(shape))
    place[longest] = (place[longest] + 1) % shape[longest]
    return values.at[tuple(place)].set(high)


def block_levels(own_key, shape, cuts, low, largest):
    def one(dim, parts):
        steps = jax.random.uniform(jax.random.fold_in(jax.random.fold_in(own_key, 6), dim), (parts,), jnp.float32, low / len(cuts), largest / len(cuts))
        return jnp.repeat(jnp.exp(steps), shape[dim] // parts).reshape((-1,) + (1,) * (len(shape) - dim - 1))

    loudness = one(*cuts[0])
    for cut in cuts[1:]:
        loudness = loudness * one(*cut)
    return loudness


def noise(rng, dims, spread, reach, cuts=(), kind=jnp.bfloat16):
    loudness = block_levels(rng, dims, cuts, -0.22, 0.18) if cuts else 1.0
    values = jax.random.normal(rng, dims, jnp.float32) * spread * loudness
    return jnp.minimum(jnp.maximum(values, -reach), reach).astype(kind)


def setup_inputs(seed: int = 0, part: int = 0) -> dict:
    key_of = jax.random.split(jax.random.key(seed), 11)
    part_keys = jax.random.split(jax.random.fold_in(key_of[10], part), 11)
    queries = draw_queries(jax.random.fold_in(jax.random.fold_in(key_of[10], part), 71), part)
    prefix_keys = draw_prefix_keys(jax.random.fold_in(jax.random.fold_in(key_of[10], part), 71), part)
    prefix_values = noise(part_keys[2], (PROMPTS, PREFIX, HEAD_DIM), 1.0, 6.0, ((1, 64),))
    stretch_keys = draw_stretch_keys(jax.random.fold_in(jax.random.fold_in(key_of[10], part), 71), part)
    stretch_values = noise(part_keys[4], (PROMPTS, STRETCH, HEAD_DIM), 1.0, 6.0, ((1, 64),))
    prefix_lengths = draw_prefix_lengths(jax.random.fold_in(jax.random.fold_in(key_of[10], part), 71), part)
    decode_queries = draw_decode_queries(jax.random.fold_in(jax.random.fold_in(key_of[10], part), 71), part)
    new_keys = draw_new_keys(jax.random.fold_in(jax.random.fold_in(key_of[10], part), 71), part)
    new_values = noise(part_keys[8], (STEPS, ROWS, HEAD_DIM), 1.0, 6.0, ((1, 2),))
    row_prompts = plant(jax.random.randint(part_keys[9], (ROWS,), 0, PROMPTS), jax.random.fold_in(part_keys[9], 1), 0, PROMPTS - 1).astype(jnp.int32)
    return {"queries": queries, "prefix_keys": prefix_keys, "prefix_values": prefix_values, "stretch_keys": stretch_keys, "stretch_values": stretch_values, "prefix_lengths": prefix_lengths, "decode_queries": decode_queries, "new_keys": new_keys, "new_values": new_values, "row_prompts": row_prompts}


def soft_weights(score_list, mask_list):
    maxima = None
    for scores, visible in zip(score_list, mask_list):
        local_max = jnp.max(jnp.where(visible, scores, -jnp.inf), axis=-1)
        maxima = local_max if maxima is None else jnp.maximum(maxima, local_max)
    weight_list = []
    denominator = None
    for scores, visible in zip(score_list, mask_list):
        weight = jnp.where(visible, jnp.exp(scores - maxima[..., None]), jnp.float32(0.0))
        partial_sum = jnp.sum(weight, axis=-1)
        denominator = partial_sum if denominator is None else denominator + partial_sum
        weight_list.append(weight.astype(jnp.bfloat16))
    return weight_list, denominator


def reference(queries, prefix_keys, prefix_values, stretch_keys, stretch_values, prefix_lengths, decode_queries, new_keys, new_values, row_prompts):
    scaling = HEAD_DIM ** -0.5
    block_len = min(512, STRETCH)

    def one_prompt(inputs):
        prompt_q, pre_k, pre_v, chk_k, chk_v, length = inputs

        def one_block(block_index):
            first_row = (block_index * block_len).astype(jnp.int32)
            query_rows = lax.dynamic_slice_in_dim(prompt_q, first_row, block_len, 0)
            query_rows = query_rows.reshape(block_len, HEADS, HEAD_DIM).astype(jnp.float32)
            pre_scores = jnp.einsum('qhd,kd->qhk', query_rows, pre_k.astype(jnp.float32)) * scaling
            chk_scores = jnp.einsum('qhd,kd->qhk', query_rows, chk_k.astype(jnp.float32)) * scaling
            query_pos = first_row + jnp.arange(block_len, dtype=jnp.int32)
            pre_seen = (jnp.arange(PREFIX, dtype=jnp.int32) < length)[None, None, :]
            chk_seen = (jnp.arange(STRETCH, dtype=jnp.int32)[None, :] <= query_pos[:, None])[:, None, :]
            weight_list, denominator = soft_weights([pre_scores, chk_scores], [pre_seen, chk_seen])
            weighted = jnp.einsum('qhk,kd->qhd', weight_list[0].astype(jnp.float32), pre_v.astype(jnp.float32))
            weighted = weighted + jnp.einsum('qhk,kd->qhd', weight_list[1].astype(jnp.float32), chk_v.astype(jnp.float32))
            result = (weighted / denominator[..., None]).astype(jnp.bfloat16)
            return result.reshape(block_len, HEADS * HEAD_DIM)

        blocks = lax.map(one_block, jnp.arange(STRETCH // block_len, dtype=jnp.int32))
        return blocks.reshape(STRETCH, HEADS * HEAD_DIM)

    prefill_out = lax.map(one_prompt, (queries, prefix_keys, prefix_values, stretch_keys, stretch_values, prefix_lengths))

    decode_rows = decode_queries.reshape(STEPS, ROWS, HEADS, HEAD_DIM).astype(jnp.float32)
    row_pre_k = prefix_keys[row_prompts].astype(jnp.float32)
    row_pre_v = prefix_values[row_prompts].astype(jnp.float32)
    row_chk_k = stretch_keys[row_prompts].astype(jnp.float32)
    row_chk_v = stretch_values[row_prompts].astype(jnp.float32)
    pre_scores = jnp.einsum('srhd,rkd->srhk', decode_rows, row_pre_k) * scaling
    chk_scores = jnp.einsum('srhd,rkd->srhk', decode_rows, row_chk_k) * scaling
    own_scores = jnp.einsum('srhd,trd->srht', decode_rows, new_keys.astype(jnp.float32)) * scaling
    row_lengths = prefix_lengths[row_prompts]
    pre_seen = (jnp.arange(PREFIX, dtype=jnp.int32)[None, :] < row_lengths[:, None])[None, :, None, :]
    chk_seen = jnp.ones((1, 1, 1, STRETCH), dtype=bool)
    step_ids = jnp.arange(STEPS, dtype=jnp.int32)
    own_seen = (step_ids[None, :] <= step_ids[:, None])[:, None, None, :]
    weight_list, denominator = soft_weights([pre_scores, chk_scores, own_scores], [pre_seen, chk_seen, own_seen])
    weighted = jnp.einsum('srhk,rkd->srhd', weight_list[0].astype(jnp.float32), row_pre_v)
    weighted = weighted + jnp.einsum('srhk,rkd->srhd', weight_list[1].astype(jnp.float32), row_chk_v)
    weighted = weighted + jnp.einsum('srht,trd->srhd', weight_list[2].astype(jnp.float32), new_values.astype(jnp.float32))
    decode_out = (weighted / denominator[..., None]).astype(jnp.bfloat16).reshape(STEPS, ROWS, HEADS * HEAD_DIM)
    return prefill_out, decode_out
```

```python
import math

import jax
import jax.numpy as jnp
from jax import lax
from jax.experimental import pallas as pl
from jax.experimental.pallas import tpu as pltpu
from jax.sharding import PartitionSpec as P

HEAD_DIM = 128
BLOCK = 128
EXP_SCALE = HEAD_DIM**-0.5 * math.log2(math.e)
NEG = -1e30
TOP = HEAD_DIM
TOT = HEAD_DIM + 8
STATE = HEAD_DIM + 16
GROUP = 16
NT = (((1,), (1,)), ((), ()))
VMEM = pl.BlockSpec(memory_space=pltpu.VMEM)
SMEM = pl.BlockSpec(memory_space=pltpu.SMEM)


def fold(state, half, at, width, scores, values_t):
    cols = pl.ds(at, width)
    top_old = state[half, TOP : TOP + 1, cols]
    total_old = state[half, TOT : TOT + 1, cols]
    top = jnp.maximum(top_old, jnp.max(scores, axis=0, keepdims=True))
    weights = jnp.exp2((scores - top) * EXP_SCALE)
    factor = jnp.exp2((top_old - top) * EXP_SCALE)
    state[half, TOP : TOP + 1, cols] = top
    state[half, TOT : TOT + 1, cols] = total_old * factor + jnp.sum(weights, axis=0, keepdims=True)
    state[half, 0:HEAD_DIM, cols] = state[half, 0:HEAD_DIM, cols] * factor + jnp.dot(
        values_t, weights.astype(jnp.bfloat16), preferred_element_type=jnp.float32
    )


def start_kernel(n_heads, steps, q_ref, dq_ref, new_ref, queries_out, state):
    q_rows = q_ref.shape[0]
    pre_cols = n_heads * q_rows
    for h in range(n_heads):
        queries_out[h * q_rows : (h + 1) * q_rows, :] = q_ref[:, h * HEAD_DIM : (h + 1) * HEAD_DIM]
    pairs = steps * n_heads
    width = pairs * GROUP
    for half in range(2):
        state[half] = jnp.zeros(state.shape[1:], jnp.float32)
        state[half, TOP : TOP + 8, :] = jnp.full((8, state.shape[2]), NEG, jnp.float32)
    for b in range(dq_ref.shape[0] // GROUP):
        rows = slice(b * GROUP, (b + 1) * GROUP)
        at = pre_cols + b * width
        block = jnp.concatenate(
            [dq_ref[rows, j * HEAD_DIM : (j + 1) * HEAD_DIM] for j in range(pairs)], axis=0
        )
        queries_out[at : at + width, :] = block
        keys = jnp.concatenate(
            [new_ref[rows, t * HEAD_DIM : (t + 1) * HEAD_DIM] for t in range(steps)], axis=0
        )
        values = jnp.concatenate(
            [new_ref[rows, (steps + t) * HEAD_DIM : (steps + t + 1) * HEAD_DIM] for t in range(steps)],
            axis=0,
        )
        scores = lax.dot_general(keys, block, NT, preferred_element_type=jnp.float32)
        key = lax.broadcasted_iota(jnp.int32, scores.shape, 0)
        col = lax.broadcasted_iota(jnp.int32, scores.shape, 1)
        seen = (key % GROUP == col % GROUP) & (key // GROUP <= col // (GROUP * n_heads))
        scores = jnp.where(seen, scores, NEG)
        fold(state, 0, at, width, scores, values.T)


def key_kernel(pre_cols, dec_width, diag, meta, *refs):
    chunks = refs[:-4]
    queries = refs[-4:-2]
    state = refs[-1]
    chunk_rows = chunks[0].shape[0]
    stretch_rows = chunk_rows - 2 * BLOCK
    keys = jnp.concatenate([r[:, :HEAD_DIM] for r in chunks], axis=0)
    values_t = jnp.concatenate([r[:, HEAD_DIM:] for r in chunks], axis=0).T
    n_pre = 2 * len(chunks)
    live = [meta[i] for i in range(n_pre)]
    stretch_live = meta[4]
    n_blocks = meta[5]
    n_live = sum(live[1:], live[0])

    def masked(scores, half, prefill):
        parts = []
        for c in range(len(chunks)):
            at = c * chunk_rows
            for i in range(2):
                dead = jnp.where(live[2 * c + i] > 0, 0.0, NEG).astype(jnp.float32)
                parts.append(scores[at + i * BLOCK : at + (i + 1) * BLOCK] + dead)
            part = scores[at + 2 * BLOCK : at + chunk_rows]
            if prefill and diag:
                row = lax.broadcasted_iota(jnp.int32, part.shape, 0)
                col = lax.broadcasted_iota(jnp.int32, part.shape, 1)
                per = stretch_rows // 2
                key_at = jnp.where(row < per, row + meta[6], row - per + meta[7])
                part = jnp.where(key_at <= col % BLOCK + meta[8 + half], part, NEG)
            elif prefill:
                part = part + jnp.where(stretch_live > 0, 0.0, NEG).astype(jnp.float32)
            parts.append(part)
        return jnp.concatenate(parts, axis=0)

    def run(half, at, width, mask, prefill):
        scores = lax.dot_general(
            keys, queries[half][pl.ds(at, width), :], NT, preferred_element_type=jnp.float32
        )
        if mask:
            scores = masked(scores, half, prefill)
        fold(state, half, at, width, scores, values_t)

    def prefill_full():
        for half in range(2):
            run(half, 0, pre_cols, False, True)

    def prefill_masked():
        def block(b, carry):
            at = pl.multiple_of(b * dec_width, BLOCK)
            for half in range(2):
                run(half, at, dec_width, True, True)
            return carry

        lax.fori_loop(0, pre_cols // dec_width, block, 0)

    if diag:
        prefill_masked()
    else:
        full = jnp.logical_and(n_live == n_pre, stretch_live > 0)
        pl.when(full)(prefill_full)
        pl.when(jnp.logical_and(jnp.logical_not(full), n_live + stretch_live > 0))(prefill_masked)

    def block(b, carry):
        at = pl.multiple_of(pre_cols + b * dec_width, BLOCK)
        for half in range(2):
            run(half, at, dec_width, True, False)
        return carry

    lax.fori_loop(0, n_blocks, block, 0)


def finish_kernel(n_heads, steps, where_ref, state, other, scatter_ref, out):
    own = state.at[0]
    top = jnp.maximum(own[TOP : TOP + 1, :], other[TOP : TOP + 1, :])
    f_own = jnp.exp2((own[TOP : TOP + 1, :] - top) * EXP_SCALE)
    f_other = jnp.exp2((other[TOP : TOP + 1, :] - top) * EXP_SCALE)
    total = own[TOT : TOT + 1, :] * f_own + other[TOT : TOT + 1, :] * f_other
    f_own = f_own / total
    f_other = f_other / total
    slots = out.shape[0]
    width = out.shape[2]
    q_rows = BLOCK
    per = width // HEAD_DIM

    def tile(at):
        cols = slice(at, at + BLOCK)
        joined = own[0:HEAD_DIM, cols] * f_own[:, cols] + other[0:HEAD_DIM, cols] * f_other[:, cols]
        return joined.T.astype(jnp.bfloat16)

    for h in range(n_heads):
        out[h // per, 0:q_rows, (h % per) * HEAD_DIM : (h % per + 1) * HEAD_DIM] = tile(h * q_rows)
    base = n_heads * q_rows
    pairs = steps * n_heads
    dec_rows = scatter_ref.shape[0]
    scatter = scatter_ref[...]
    each = BLOCK // GROUP
    n_blocks = dec_rows // GROUP
    for s in range(steps):
        slot = where_ref[s]
        for h0 in range(0, n_heads, each):
            tiles = [tile(base + b * pairs * GROUP + (s * n_heads + h0) * GROUP) for b in range(n_blocks)]
            for e in range(each):
                rows = jnp.concatenate([t[e * GROUP : (e + 1) * GROUP, :] for t in tiles], axis=0)
                put = jnp.dot(scatter, rows, preferred_element_type=jnp.float32).astype(jnp.bfloat16)
                h = h0 + e
                at = q_rows + (h // per) * dec_rows
                out[slot, at : at + dec_rows, (h % per) * HEAD_DIM : (h % per + 1) * HEAD_DIM] = put


def shift(n, by):
    return [(i, (i + by) % n) for i in range(n)]


def local(
    queries,
    prefix_keys,
    prefix_values,
    stretch_keys,
    stretch_values,
    prefix_lengths,
    decode_queries,
    new_keys,
    new_values,
    row_prompts,
):
    prompts, q_rows, width = queries.shape
    heads_dev = width // HEAD_DIM
    pre_rows = prefix_keys.shape[1]
    chk_rows = stretch_keys.shape[1]
    steps, row_dev, _ = decode_queries.shape
    n_x = lax.axis_size("head")
    n_z = lax.axis_size("blk")
    n_heads = heads_dev * n_x
    x = lax.axis_index("head")
    z = lax.axis_index("blk")
    rep = lax.axis_index("rep")
    assert prompts == n_x == 4 and pre_rows == BLOCK and q_rows == BLOCK and steps == n_x
    swap = [(0, 1), (1, 0)]

    message = jnp.concatenate(
        [
            jnp.concatenate([prefix_keys, prefix_values], axis=2),
            jnp.concatenate([stretch_keys, stretch_values], axis=2),
            queries,
        ],
        axis=1,
    )
    got = []
    for k in range(n_x):
        piece = lax.dynamic_index_in_dim(message, (x + k) % n_x, 0, keepdims=False)
        got.append(piece if k == 0 else lax.ppermute(piece, "head", shift(n_x, k)))
    cut = pre_rows + chk_rows

    def chunk(i, j):
        return jnp.concatenate(
            [got[i][:pre_rows], got[j][:pre_rows], got[i][pre_rows:cut], got[j][pre_rows:cut]], axis=0
        )

    chunks = [chunk(0, 1), chunk(2, 3)]
    q_mine = jnp.concatenate([g[cut:] for g in got], axis=1)

    rows_other = lax.ppermute(row_prompts, "rep", swap)
    match = row_prompts == x
    place = jnp.sum(
        (jnp.arange(row_dev)[None, :] < jnp.arange(row_dev)[:, None]) & match[None, :], axis=1
    )
    pack = ((place[None, :] == jnp.arange(row_dev)[:, None]) & match[None, :]).astype(jnp.bfloat16)
    most = jnp.maximum(jnp.sum(match), jnp.sum(rows_other == x)).astype(jnp.int32)
    dec_blocks = (most + GROUP - 1) // GROUP
    flat = jnp.concatenate(
        [decode_queries[s] for s in range(steps)]
        + [new_keys[s] for s in range(steps)]
        + [new_values[s] for s in range(steps)],
        axis=1,
    )
    packed = jnp.dot(pack, flat, preferred_element_type=jnp.float32).astype(jnp.bfloat16)
    dec_width = steps * n_heads * GROUP
    pre_cols = n_heads * q_rows
    cols = pre_cols + row_dev // GROUP * dec_width

    state_shape = jax.ShapeDtypeStruct((2, STATE, cols), jnp.float32)
    params = pltpu.CompilerParams(vmem_limit_bytes=32 << 20)
    q_own, state = pl.pallas_call(
        lambda *refs: start_kernel(n_heads, steps, *refs),
        name="start",
        out_shape=(jax.ShapeDtypeStruct((cols, HEAD_DIM), jnp.bfloat16), state_shape),
        in_specs=[VMEM] * 3,
        out_specs=(VMEM,) * 2,
        compiler_params=params,
        cost_estimate=pl.CostEstimate(flops=1 << 28, bytes_accessed=1 << 21, transcendentals=0),
    )(q_mine, packed[:, : steps * n_heads * HEAD_DIM], packed[:, steps * n_heads * HEAD_DIM :])
    q_other = lax.ppermute(q_own, "rep", swap)

    length = jnp.sum(jnp.where(jnp.arange(prompts) == x, prefix_lengths, 0))
    from_x = (x - jnp.arange(n_x)) % n_x

    def meta_of(plane, first, count):
        live = (((plane * n_x + from_x) * pre_rows) < length).astype(jnp.int32)
        pick = lax.dynamic_slice_in_dim(live, first, count) if count < n_x else live
        pick = jnp.concatenate([pick, jnp.ones((n_x - count,), jnp.int32)])
        at = lax.dynamic_slice_in_dim(from_x, first, 2) * chk_rows
        tail = jnp.stack(
            [(plane < z).astype(jnp.int32), dec_blocks, at[0], at[1], rep * q_rows, (1 - rep) * q_rows]
        )
        return jnp.concatenate([pick, tail]).astype(jnp.int32)

    def visit(state, parts, meta, diag):
        rows = sum(p.shape[0] for p in parts)
        flops = 4 * rows * HEAD_DIM * 3 * pre_cols
        return pl.pallas_call(
            lambda *refs: key_kernel(pre_cols, dec_width, diag, *refs),
            name="visit",
            out_shape=state_shape,
            in_specs=[SMEM] + [VMEM] * (len(parts) + 3),
            out_specs=VMEM,
            input_output_aliases={len(parts) + 3: 0},
            compiler_params=params,
            cost_estimate=pl.CostEstimate(flops=flops, bytes_accessed=1 << 20, transcendentals=0),
        )(meta, *parts, q_own, q_other, state)

    step_dir = 1 - 2 * rep
    up = [((i * 2), ((i + 1) % n_z) * 2) for i in range(n_z)]
    down = [((i * 2 + 1), ((i - 1) % n_z) * 2 + 1) for i in range(n_z)]

    def one_of_two(pair):
        return jnp.where(rep == 0, pair[0], pair[1])

    half = n_z // 2
    home = one_of_two(chunks)
    travel = [lax.ppermute(c, ("blk", "rep"), up + down) for c in chunks]
    state = visit(state, [home], meta_of(z, 2 * rep, 2), True)
    for s in range(1, half):
        here = travel
        if s + 1 < half:
            travel = [lax.ppermute(c, ("blk", "rep"), up + down) for c in here]
        else:
            travel = [lax.ppermute(one_of_two(here), ("blk", "rep"), up + down)]
        state = visit(state, here, meta_of((z - step_dir * s) % n_z, 0, n_x), False)
    state = visit(state, travel, meta_of((z + half) % n_z, 2 * rep, 2), False)

    theirs = lax.ppermute(state[1], "rep", swap)
    where = (x - jnp.arange(steps, dtype=jnp.int32)) % n_x
    dec_tall = row_dev * n_heads // heads_dev
    ready = pl.pallas_call(
        lambda *refs: finish_kernel(n_heads, steps, *refs),
        name="finish",
        out_shape=jax.ShapeDtypeStruct((n_x, q_rows + dec_tall, width), jnp.bfloat16),
        in_specs=[SMEM] + [VMEM] * 3,
        out_specs=VMEM,
        compiler_params=params,
        cost_estimate=pl.CostEstimate(flops=1 << 28, bytes_accessed=1 << 21, transcendentals=0),
    )(where, state, theirs, pack.T)

    back = [ready[0]] + [lax.ppermute(ready[k], "head", shift(n_x, -k)) for k in range(1, n_x)]
    prefill_out = jnp.roll(jnp.stack([b[:q_rows] for b in back]), x, axis=0)
    mine = back[0][q_rows:]
    for b in back[1:]:
        mine = mine + b[q_rows:]
    around = [mine] + [lax.ppermute(mine, "head", shift(n_x, -k)) for k in range(1, n_x)]
    decoded = jnp.roll(jnp.stack(around), x, axis=0)
    decode_out = jnp.concatenate(
        [decoded[:, i * row_dev : (i + 1) * row_dev] for i in range(n_x)], axis=2
    )
    return (prefill_out, decode_out)


def solution(mesh):
    placed = (
        P("groups", ("blk", "rep"), "head"),
        P("groups", ("blk", "head"), None),
        P("groups", ("blk", "head"), None),
        P("groups", ("blk", "head"), None),
        P("groups", ("blk", "head"), None),
        P("groups"),
        P("groups", "rep", None),
        P("groups", "rep", None),
        P("groups", "rep", None),
        P(("groups", "rep")),
    )
    return jax.shard_map(
        local,
        mesh=mesh,
        in_specs=placed,
        out_specs=(P("groups", ("blk", "rep"), "head"), P("groups", "rep", None)),
        check_vma=False,
    )
```

```python
import math

import jax
import jax.numpy as jnp
from jax import lax
from jax.experimental import pallas as pl
from jax.experimental.pallas import tpu as pltpu
from jax.sharding import PartitionSpec as P


HEAD_DIM = 128
BLOCK = 128
EXP_SCALE = HEAD_DIM**-0.5 * math.log2(math.e)
NEG = -1e30
TOP = HEAD_DIM
TOT = HEAD_DIM + 8
STATE = HEAD_DIM + 16
GROUP = 16
NT = (((1,), (1,)), ((), ()))
VMEM = pl.BlockSpec(memory_space=pltpu.VMEM)
SMEM = pl.BlockSpec(memory_space=pltpu.SMEM)


def fold(state, half, at, width, scores, values_t):
    cols = pl.ds(at, width)
    top_old = state[half, TOP : TOP + 1, cols]
    total_old = state[half, TOT : TOT + 1, cols]
    top = jnp.maximum(top_old, jnp.max(scores, axis=0, keepdims=True))
    weights = jnp.exp2((scores - top) * EXP_SCALE)
    factor = jnp.exp2((top_old - top) * EXP_SCALE)
    state[half, TOP : TOP + 1, cols] = top
    state[half, TOT : TOT + 1, cols] = total_old * factor + jnp.sum(weights, axis=0, keepdims=True)
    state[half, 0:HEAD_DIM, cols] = state[half, 0:HEAD_DIM, cols] * factor + jnp.dot(
        values_t, weights.astype(jnp.bfloat16), preferred_element_type=jnp.float32
    )


def start_kernel(n_heads, steps, q_ref, dq_ref, new_ref, queries_out, state):
    q_rows = q_ref.shape[0]
    pre_cols = n_heads * q_rows
    for h in range(n_heads):
        queries_out[h * q_rows : (h + 1) * q_rows, :] = q_ref[:, h * HEAD_DIM : (h + 1) * HEAD_DIM]
    pairs = steps * n_heads
    width = pairs * GROUP
    for half in range(2):
        state[half] = jnp.zeros(state.shape[1:], jnp.float32)
        state[half, TOP : TOP + 8, :] = jnp.full((8, state.shape[2]), NEG, jnp.float32)
    for b in range(dq_ref.shape[0] // GROUP):
        rows = slice(b * GROUP, (b + 1) * GROUP)
        at = pre_cols + b * width
        block = jnp.concatenate(
            [dq_ref[rows, j * HEAD_DIM : (j + 1) * HEAD_DIM] for j in range(pairs)], axis=0
        )
        queries_out[at : at + width, :] = block
        keys = jnp.concatenate(
            [new_ref[rows, t * HEAD_DIM : (t + 1) * HEAD_DIM] for t in range(steps)], axis=0
        )
        values = jnp.concatenate(
            [new_ref[rows, (steps + t) * HEAD_DIM : (steps + t + 1) * HEAD_DIM] for t in range(steps)],
            axis=0,
        )
        scores = lax.dot_general(keys, block, NT, preferred_element_type=jnp.float32)
        key = lax.broadcasted_iota(jnp.int32, scores.shape, 0)
        col = lax.broadcasted_iota(jnp.int32, scores.shape, 1)
        seen = (key % GROUP == col % GROUP) & (key // GROUP <= col // (GROUP * n_heads))
        scores = jnp.where(seen, scores, NEG)
        fold(state, 0, at, width, scores, values.T)


def key_kernel(pre_cols, dec_width, visit, diag, meta, *refs):
    chunks = refs[:-3]
    queries = refs[-3]
    state = refs[-1]
    chunk_rows = chunks[0].shape[0]
    stretch_rows = chunk_rows - 2 * BLOCK
    keys = jnp.concatenate([r[:, :HEAD_DIM] for r in chunks], axis=0)
    values_t = jnp.concatenate([r[:, HEAD_DIM:] for r in chunks], axis=0).T
    n_pre = 2 * len(chunks)
    live = [meta[visit, i] for i in range(n_pre)]
    stretch_live = meta[visit, 4]
    n_blocks = meta[visit, 5]
    n_live = sum(live[1:], live[0])
    pre_blocks = pre_cols // dec_width

    def masked(scores, half, prefill):
        parts = []
        for c in range(len(chunks)):
            at = c * chunk_rows
            for i in range(2):
                dead = jnp.where(live[2 * c + i] > 0, 0.0, NEG).astype(jnp.float32)
                parts.append(scores[at + i * BLOCK : at + (i + 1) * BLOCK] + dead)
            part = scores[at + 2 * BLOCK : at + chunk_rows]
            if diag:
                row = lax.broadcasted_iota(jnp.int32, part.shape, 0)
                col = lax.broadcasted_iota(jnp.int32, part.shape, 1)
                per = stretch_rows // 2
                key_at = jnp.where(row < per, row + meta[visit, 6], row - per + meta[visit, 7])
                last = jnp.where(prefill, 0, 4 * stretch_rows) + meta[visit, 8 + half]
                part = jnp.where(key_at <= col % BLOCK + last, part, NEG)
            else:
                hidden = jnp.logical_and(prefill, stretch_live == 0)
                part = part + jnp.where(hidden, NEG, 0.0).astype(jnp.float32)
            parts.append(part)
        return jnp.concatenate(parts, axis=0)

    def scores_of(half, at, width):
        return lax.dot_general(
            keys, queries[half, pl.ds(at, width), :], NT, preferred_element_type=jnp.float32
        )

    first = 0
    if not diag:
        full = jnp.logical_and(n_live == n_pre, stretch_live > 0)

        @pl.when(full)
        def _():
            def whole(half, carry):
                fold(state, half, 0, pre_cols, scores_of(half, 0, pre_cols), values_t)
                return carry

            lax.fori_loop(0, 2, whole, 0)

        skip = jnp.logical_or(full, n_live + stretch_live == 0)
        first = jnp.where(skip, 2 * pre_blocks, 0)

    def block(j, carry):
        half = j % 2
        at = pl.multiple_of(j // 2 * dec_width, BLOCK)
        scores = masked(scores_of(half, at, dec_width), half, j < 2 * pre_blocks)
        fold(state, half, at, dec_width, scores, values_t)
        return carry

    lax.fori_loop(first, 2 * (pre_blocks + n_blocks), block, 0)


def finish_kernel(n_heads, steps, where_ref, state, other, scatter_ref, out):
    own = state.at[0]
    top = jnp.maximum(own[TOP : TOP + 1, :], other[TOP : TOP + 1, :])
    f_own = jnp.exp2((own[TOP : TOP + 1, :] - top) * EXP_SCALE)
    f_other = jnp.exp2((other[TOP : TOP + 1, :] - top) * EXP_SCALE)
    total = own[TOT : TOT + 1, :] * f_own + other[TOT : TOT + 1, :] * f_other
    f_own = f_own / total
    f_other = f_other / total
    width = out.shape[2]
    q_rows = BLOCK
    per = width // HEAD_DIM

    def tile(at):
        cols = slice(at, at + BLOCK)
        joined = own[0:HEAD_DIM, cols] * f_own[:, cols] + other[0:HEAD_DIM, cols] * f_other[:, cols]
        return joined.T.astype(jnp.bfloat16)

    for h in range(n_heads):
        out[h // per, 0:q_rows, (h % per) * HEAD_DIM : (h % per + 1) * HEAD_DIM] = tile(h * q_rows)
    base = n_heads * q_rows
    pairs = steps * n_heads
    dec_rows = scatter_ref.shape[0]
    scatter = scatter_ref[...]
    each = BLOCK // GROUP
    n_blocks = dec_rows // GROUP
    for s in range(steps):
        slot = where_ref[s]
        for h0 in range(0, n_heads, each):
            tiles = [tile(base + b * pairs * GROUP + (s * n_heads + h0) * GROUP) for b in range(n_blocks)]
            for e in range(each):
                rows = jnp.concatenate([t[e * GROUP : (e + 1) * GROUP, :] for t in tiles], axis=0)
                put = jnp.dot(scatter, rows, preferred_element_type=jnp.float32).astype(jnp.bfloat16)
                h = h0 + e
                at = q_rows + (h // per) * dec_rows
                out[slot, at : at + dec_rows, (h % per) * HEAD_DIM : (h % per + 1) * HEAD_DIM] = put


def shift(n, by):
    return [(i, (i + by) % n) for i in range(n)]


def local(
    queries,
    prefix_keys,
    prefix_values,
    stretch_keys,
    stretch_values,
    prefix_lengths,
    decode_queries,
    new_keys,
    new_values,
    row_prompts,
):
    prompts, q_rows, width = queries.shape
    heads_dev = width // HEAD_DIM
    pre_rows = prefix_keys.shape[1]
    chk_rows = stretch_keys.shape[1]
    steps, row_dev, _ = decode_queries.shape
    n_x = lax.axis_size("head")
    n_z = lax.axis_size("blk")
    n_heads = heads_dev * n_x
    x = lax.axis_index("head")
    z = lax.axis_index("blk")
    rep = lax.axis_index("rep")
    assert prompts == n_x == 4 and pre_rows == BLOCK and q_rows == BLOCK and steps == n_x
    swap = [(0, 1), (1, 0)]

    message = jnp.concatenate(
        [
            jnp.concatenate([prefix_keys, prefix_values], axis=2),
            jnp.concatenate([stretch_keys, stretch_values], axis=2),
            queries,
        ],
        axis=1,
    )
    got = []
    for k in range(n_x):
        piece = lax.dynamic_index_in_dim(message, (x + k) % n_x, 0, keepdims=False)
        got.append(piece if k == 0 else lax.ppermute(piece, "head", shift(n_x, k)))
    cut = pre_rows + chk_rows

    def chunk(i, j):
        return jnp.concatenate(
            [got[i][:pre_rows], got[j][:pre_rows], got[i][pre_rows:cut], got[j][pre_rows:cut]], axis=0
        )

    chunks = [chunk(0, 1), chunk(2, 3)]
    q_mine = jnp.concatenate([g[cut:] for g in got], axis=1)

    rows_other = lax.ppermute(row_prompts, "rep", swap)
    match = row_prompts == x
    place = jnp.sum(
        (jnp.arange(row_dev)[None, :] < jnp.arange(row_dev)[:, None]) & match[None, :], axis=1
    )
    pack = ((place[None, :] == jnp.arange(row_dev)[:, None]) & match[None, :]).astype(jnp.bfloat16)
    most = jnp.maximum(jnp.sum(match), jnp.sum(rows_other == x)).astype(jnp.int32)
    dec_blocks = (most + GROUP - 1) // GROUP
    flat = jnp.concatenate(
        [decode_queries[s] for s in range(steps)]
        + [new_keys[s] for s in range(steps)]
        + [new_values[s] for s in range(steps)],
        axis=1,
    )
    packed = jnp.dot(pack, flat, preferred_element_type=jnp.float32).astype(jnp.bfloat16)
    dec_width = steps * n_heads * GROUP
    pre_cols = n_heads * q_rows
    cols = pre_cols + row_dev // GROUP * dec_width

    state_shape = jax.ShapeDtypeStruct((2, STATE, cols), jnp.float32)
    params = pltpu.CompilerParams(vmem_limit_bytes=32 << 20)
    q_own, state = pl.pallas_call(
        lambda *refs: start_kernel(n_heads, steps, *refs),
        name="start",
        out_shape=(jax.ShapeDtypeStruct((cols, HEAD_DIM), jnp.bfloat16), state_shape),
        in_specs=[VMEM] * 3,
        out_specs=(VMEM,) * 2,
        compiler_params=params,
        cost_estimate=pl.CostEstimate(flops=1 << 28, bytes_accessed=1 << 21, transcendentals=0),
    )(q_mine, packed[:, : steps * n_heads * HEAD_DIM], packed[:, steps * n_heads * HEAD_DIM :])
    q_other = lax.ppermute(q_own, "rep", swap)

    q_all = jnp.stack([q_own, q_other])

    half = n_z // 2
    length = jnp.sum(jnp.where(jnp.arange(prompts) == x, prefix_lengths, 0))
    visit_at = lax.broadcasted_iota(jnp.int32, (half + 1, 16), 0)
    item = lax.broadcasted_iota(jnp.int32, (half + 1, 16), 1)
    step_dir = 1 - 2 * rep
    plane = (z - step_dir * visit_at + n_z) % n_z
    slot = jnp.where(item < n_x, item, item - 6) + jnp.where(visit_at % half == 0, 2 * rep, 0)
    from_x = (x - slot + 2 * n_x) % n_x
    meta = jnp.where(item < n_x, (plane * n_x + from_x) * pre_rows < length, plane < z).astype(jnp.int32)
    meta = jnp.where(item == 5, dec_blocks, meta)
    meta = jnp.where((item == 6) | (item == 7), from_x * chk_rows, meta)
    meta = jnp.where(item == 8, rep * q_rows, jnp.where(item == 9, (1 - rep) * q_rows, meta))

    def visit(state, parts, index, diag):
        rows = sum(p.shape[0] for p in parts)
        flops = 4 * rows * HEAD_DIM * 3 * pre_cols
        return pl.pallas_call(
            lambda *refs: key_kernel(pre_cols, dec_width, index, diag, *refs),
            name="visit",
            out_shape=state_shape,
            in_specs=[SMEM] + [VMEM] * (len(parts) + 2),
            out_specs=VMEM,
            input_output_aliases={len(parts) + 2: 0},
            compiler_params=params,
            cost_estimate=pl.CostEstimate(flops=flops, bytes_accessed=1 << 20, transcendentals=0),
        )(meta, *parts, q_all, state)

    up = [((i * 2), ((i + 1) % n_z) * 2) for i in range(n_z)]
    down = [((i * 2 + 1), ((i - 1) % n_z) * 2 + 1) for i in range(n_z)]

    def hop(parts):
        moved = []
        for part in parts:
            moved.append(lax.ppermute(part, ("blk", "rep"), up + down))
        return moved

    def one_of_two(pair):
        return jnp.where(rep == 0, pair[0], pair[1])

    travel = hop(chunks)
    state = visit(state, [one_of_two(chunks)], 0, True)
    for s in range(1, half):
        here = travel
        travel = hop(here if s + 1 < half else [one_of_two(here)])
        state = visit(state, here, s, False)
    state = visit(state, travel, half, False)

    theirs = lax.ppermute(state[1], "rep", swap)
    where = (x - jnp.arange(steps, dtype=jnp.int32)) % n_x
    dec_tall = row_dev * n_heads // heads_dev
    ready = pl.pallas_call(
        lambda *refs: finish_kernel(n_heads, steps, *refs),
        name="finish",
        out_shape=jax.ShapeDtypeStruct((n_x, q_rows + dec_tall, width), jnp.bfloat16),
        in_specs=[SMEM] + [VMEM] * 3,
        out_specs=VMEM,
        compiler_params=params,
        cost_estimate=pl.CostEstimate(flops=1 << 28, bytes_accessed=1 << 21, transcendentals=0),
    )(where, state, theirs, pack.T)

    back = [ready[0]] + [lax.ppermute(ready[k], "head", shift(n_x, -k)) for k in range(1, n_x)]
    prefill_out = jnp.roll(jnp.stack([b[:q_rows] for b in back]), x, axis=0)
    mine = back[0][q_rows:]
    for b in back[1:]:
        mine = mine + b[q_rows:]
    around = [mine] + [lax.ppermute(mine, "head", shift(n_x, -k)) for k in range(1, n_x)]
    decoded = jnp.roll(jnp.stack(around), x, axis=0)
    decode_out = jnp.concatenate(
        [decoded[:, i * row_dev : (i + 1) * row_dev] for i in range(n_x)], axis=2
    )
    return (prefill_out, decode_out)


def solution(mesh):
    placed = (
        P("groups", ("blk", "rep"), "head"),
        P("groups", ("blk", "head"), None),
        P("groups", ("blk", "head"), None),
        P("groups", ("blk", "head"), None),
        P("groups", ("blk", "head"), None),
        P("groups"),
        P("groups", "rep", None),
        P("groups", "rep", None),
        P("groups", "rep", None),
        P(("groups", "rep")),
    )
    return jax.shard_map(
        local,
        mesh=mesh,
        in_specs=placed,
        out_specs=(P("groups", ("blk", "rep"), "head"), P("groups", "rep", None)),
        check_vma=False,
    )
```

```python
import math

import jax
import jax.numpy as jnp
from jax import lax
from jax.experimental import pallas as pl
from jax.experimental.pallas import tpu as pltpu
from jax.sharding import PartitionSpec as P


HEAD_DIM = 128
BLOCK = 128
EXP_SCALE = HEAD_DIM**-0.5 * math.log2(math.e)
NEG = -1e30
TOP = HEAD_DIM
TOT = HEAD_DIM + 8
STATE = HEAD_DIM + 16
GROUP = 16
NT = (((1,), (1,)), ((), ()))
VMEM = pl.BlockSpec(memory_space=pltpu.VMEM)
SMEM = pl.BlockSpec(memory_space=pltpu.SMEM)


def fold(state, half, at, width, scores, values_t):
    cols = pl.ds(at, width)
    top_old = state[half, TOP : TOP + 1, cols]
    total_old = state[half, TOT : TOT + 1, cols]
    top = jnp.maximum(top_old, jnp.max(scores, axis=0, keepdims=True))
    weights = jnp.exp2((scores - top) * EXP_SCALE)
    factor = jnp.exp2((top_old - top) * EXP_SCALE)
    state[half, TOP : TOP + 1, cols] = top
    state[half, TOT : TOT + 1, cols] = total_old * factor + jnp.sum(weights, axis=0, keepdims=True)
    state[half, 0:HEAD_DIM, cols] = state[half, 0:HEAD_DIM, cols] * factor + jnp.dot(
        values_t, weights.astype(jnp.bfloat16), preferred_element_type=jnp.float32
    )


def start_kernel(n_heads, steps, x_ref, q_ref, dq_ref, nk_ref, nv_ref, row_ref, col_ref, queries_out, state, spread):
    q_rows = q_ref.shape[0]
    n_rows = dq_ref.shape[1]
    pre_cols = n_heads * q_rows
    x = x_ref[0]
    for h in range(n_heads):
        queries_out[h * q_rows : (h + 1) * q_rows, :] = q_ref[:, h * HEAD_DIM : (h + 1) * HEAD_DIM]
    for half in range(2):
        state[half] = jnp.zeros(state.shape[1:], jnp.float32)
        state[half, TOP : TOP + 8, :] = jnp.full((8, state.shape[2]), NEG, jnp.float32)

    lo = lax.broadcasted_iota(jnp.int32, (n_rows, n_rows), 0)
    hi = lax.broadcasted_iota(jnp.int32, (n_rows, n_rows), 1)
    hit_row = jnp.broadcast_to(row_ref[...], (n_rows, n_rows)) == x
    hit_col = jnp.broadcast_to(col_ref[...], (n_rows, n_rows)) == x
    ones_row = jnp.where(hit_row, 1.0, 0.0)
    ones_col = jnp.where(hit_col, 1.0, 0.0)
    place_row = jnp.dot(ones_row, jnp.where(lo < hi, 1.0, 0.0), preferred_element_type=jnp.float32)
    place_col = jnp.dot(jnp.where(hi < lo, 1.0, 0.0), ones_col, preferred_element_type=jnp.float32)
    pack = jnp.where(jnp.logical_and(hit_row, place_row.astype(jnp.int32) == lo), 1.0, 0.0).astype(jnp.bfloat16)
    spread[...] = jnp.where(jnp.logical_and(hit_col, place_col.astype(jnp.int32) == hi), 1.0, 0.0).astype(
        jnp.bfloat16
    )
    count = jnp.sum(ones_row[0:1, :], axis=1, keepdims=True)
    total = queries_out.shape[0]
    queries_out[total - GROUP : total, :] = jnp.broadcast_to(count, (GROUP, HEAD_DIM)).astype(jnp.bfloat16)

    def packed(ref, t, at):
        rows = ref[t, :, at : at + HEAD_DIM]
        return jnp.dot(pack, rows, preferred_element_type=jnp.float32).astype(jnp.bfloat16)

    tiles = [packed(dq_ref, s, h * HEAD_DIM) for s in range(steps) for h in range(n_heads)]
    new_k = [packed(nk_ref, t, 0) for t in range(steps)]
    new_v = [packed(nv_ref, t, 0) for t in range(steps)]
    width = steps * n_heads * GROUP
    for b in range(n_rows // GROUP):
        rows = slice(b * GROUP, (b + 1) * GROUP)
        at = pre_cols + b * width
        block = jnp.concatenate([t[rows] for t in tiles], axis=0)
        queries_out[at : at + width, :] = block
        keys = jnp.concatenate([t[rows] for t in new_k], axis=0)
        values = jnp.concatenate([t[rows] for t in new_v], axis=0)
        scores = lax.dot_general(keys, block, NT, preferred_element_type=jnp.float32)
        key = lax.broadcasted_iota(jnp.int32, scores.shape, 0)
        col = lax.broadcasted_iota(jnp.int32, scores.shape, 1)
        seen = (key % GROUP == col % GROUP) & (key // GROUP <= col // (GROUP * n_heads))
        scores = jnp.where(seen, scores, NEG)
        fold(state, 0, at, width, scores, values.T)


def key_kernel(pre_cols, dec_width, visit, diag, meta, *refs):
    chunks = refs[:-3]
    queries = refs[-3]
    state = refs[-1]
    chunk_rows = chunks[0].shape[0]
    stretch_rows = chunk_rows - 2 * BLOCK
    keys = jnp.concatenate([r[:, :HEAD_DIM] for r in chunks], axis=0)
    values_t = jnp.concatenate([r[:, HEAD_DIM:] for r in chunks], axis=0).T
    n_pre = 2 * len(chunks)
    live = [meta[visit, i] for i in range(n_pre)]
    stretch_live = meta[visit, 4]
    total = queries.shape[1]
    most = jnp.max(queries[:, total - GROUP : total, :].astype(jnp.float32)).astype(jnp.int32)
    n_blocks = (most + GROUP - 1) // GROUP
    n_live = sum(live[1:], live[0])
    pre_blocks = pre_cols // dec_width

    def masked(scores, half, prefill):
        parts = []
        for c in range(len(chunks)):
            at = c * chunk_rows
            for i in range(2):
                dead = jnp.where(live[2 * c + i] > 0, 0.0, NEG).astype(jnp.float32)
                parts.append(scores[at + i * BLOCK : at + (i + 1) * BLOCK] + dead)
            part = scores[at + 2 * BLOCK : at + chunk_rows]
            if diag:
                row = lax.broadcasted_iota(jnp.int32, part.shape, 0)
                col = lax.broadcasted_iota(jnp.int32, part.shape, 1)
                per = stretch_rows // 2
                key_at = jnp.where(row < per, row + meta[visit, 6], row - per + meta[visit, 7])
                last = jnp.where(prefill, 0, 4 * stretch_rows) + meta[visit, 8 + half]
                part = jnp.where(key_at <= col % BLOCK + last, part, NEG)
            else:
                hidden = jnp.logical_and(prefill, stretch_live == 0)
                part = part + jnp.where(hidden, NEG, 0.0).astype(jnp.float32)
            parts.append(part)
        return jnp.concatenate(parts, axis=0)

    def scores_of(half, at, width):
        return lax.dot_general(
            keys, queries[half, pl.ds(at, width), :], NT, preferred_element_type=jnp.float32
        )

    first = 0
    if len(chunks) > 1:
        full = jnp.logical_and(n_live == n_pre, stretch_live > 0)

        @pl.when(full)
        def _():
            def whole(half, carry):
                fold(state, half, 0, pre_cols, scores_of(half, 0, pre_cols), values_t)
                return carry

            lax.fori_loop(0, 2, whole, 0)

        first = jnp.where(full, 2 * pre_blocks, 0)
    if not diag:
        first = jnp.where(n_live + stretch_live == 0, 2 * pre_blocks, first)

    def block(j, carry):
        half = j % 2
        at = pl.multiple_of(j // 2 * dec_width, BLOCK)
        scores = masked(scores_of(half, at, dec_width), half, j < 2 * pre_blocks)
        fold(state, half, at, dec_width, scores, values_t)
        return carry

    lax.fori_loop(first, 2 * (pre_blocks + n_blocks), block, 0)


def finish_kernel(n_heads, steps, where_ref, state, other, scatter_ref, out):
    own = state.at[0]
    top = jnp.maximum(own[TOP : TOP + 1, :], other[TOP : TOP + 1, :])
    f_own = jnp.exp2((own[TOP : TOP + 1, :] - top) * EXP_SCALE)
    f_other = jnp.exp2((other[TOP : TOP + 1, :] - top) * EXP_SCALE)
    total = own[TOT : TOT + 1, :] * f_own + other[TOT : TOT + 1, :] * f_other
    f_own = f_own / total
    f_other = f_other / total
    width = out.shape[2]
    q_rows = BLOCK
    per = width // HEAD_DIM

    def tile(at):
        cols = slice(at, at + BLOCK)
        joined = own[0:HEAD_DIM, cols] * f_own[:, cols] + other[0:HEAD_DIM, cols] * f_other[:, cols]
        return joined.T.astype(jnp.bfloat16)

    for h in range(n_heads):
        out[where_ref[h // per], 0:q_rows, (h % per) * HEAD_DIM : (h % per + 1) * HEAD_DIM] = tile(h * q_rows)
    base = n_heads * q_rows
    pairs = steps * n_heads
    dec_rows = scatter_ref.shape[0]
    scatter = scatter_ref[...]
    each = BLOCK // GROUP
    n_blocks = dec_rows // GROUP
    for s in range(steps):
        for h0 in range(0, n_heads, each):
            tiles = [tile(base + b * pairs * GROUP + (s * n_heads + h0) * GROUP) for b in range(n_blocks)]
            for e in range(each):
                rows = jnp.concatenate([t[e * GROUP : (e + 1) * GROUP, :] for t in tiles], axis=0)
                put = jnp.dot(scatter, rows, preferred_element_type=jnp.float32).astype(jnp.bfloat16)
                h = h0 + e
                at = q_rows + (h // per) * dec_rows
                out[s, at : at + dec_rows, (h % per) * HEAD_DIM : (h % per + 1) * HEAD_DIM] = put


def shift(n, by):
    return [(i, (i + by) % n) for i in range(n)]


def local(
    queries,
    prefix_keys,
    prefix_values,
    stretch_keys,
    stretch_values,
    prefix_lengths,
    decode_queries,
    new_keys,
    new_values,
    row_prompts,
):
    prompts, q_rows, width = queries.shape
    heads_dev = width // HEAD_DIM
    pre_rows = prefix_keys.shape[1]
    chk_rows = stretch_keys.shape[1]
    steps, row_dev, _ = decode_queries.shape
    n_x = lax.axis_size("head")
    n_z = lax.axis_size("blk")
    n_heads = heads_dev * n_x
    x = lax.axis_index("head")
    z = lax.axis_index("blk")
    rep = lax.axis_index("rep")
    assert prompts == n_x == 4 and pre_rows == BLOCK and q_rows == BLOCK and steps == n_x
    swap = [(0, 1), (1, 0)]

    message = jnp.concatenate(
        [
            jnp.concatenate([prefix_keys, prefix_values], axis=2),
            jnp.concatenate([stretch_keys, stretch_values], axis=2),
            queries,
        ],
        axis=1,
    )
    got = []
    for k in range(n_x):
        piece = lax.dynamic_index_in_dim(message, (x + k) % n_x, 0, keepdims=False)
        got.append(piece if k == 0 else lax.ppermute(piece, "head", shift(n_x, k)))
    cut = pre_rows + chk_rows

    def chunk(i, j):
        return jnp.concatenate(
            [got[i][:pre_rows], got[j][:pre_rows], got[i][pre_rows:cut], got[j][pre_rows:cut]], axis=0
        )

    chunks = [chunk(0, 1), chunk(2, 3)]
    q_mine = jnp.concatenate([g[cut:] for g in got], axis=1)

    dec_width = steps * n_heads * GROUP
    pre_cols = n_heads * q_rows
    cols = pre_cols + row_dev // GROUP * dec_width

    state_shape = jax.ShapeDtypeStruct((2, STATE, cols), jnp.float32)
    params = pltpu.CompilerParams(vmem_limit_bytes=32 << 20)
    q_own, state, spread = pl.pallas_call(
        lambda *refs: start_kernel(n_heads, steps, *refs),
        name="start",
        out_shape=(
            jax.ShapeDtypeStruct((cols + GROUP, HEAD_DIM), jnp.bfloat16),
            state_shape,
            jax.ShapeDtypeStruct((row_dev, row_dev), jnp.bfloat16),
        ),
        in_specs=[SMEM] + [VMEM] * 6,
        out_specs=(VMEM,) * 3,
        compiler_params=params,
        cost_estimate=pl.CostEstimate(flops=1 << 28, bytes_accessed=1 << 21, transcendentals=0),
    )(x[None], q_mine, decode_queries, new_keys, new_values, row_prompts[None, :], row_prompts[:, None])
    q_other = lax.ppermute(q_own, "rep", swap)

    q_all = jnp.stack([q_own, q_other])

    half = n_z // 2
    length = jnp.sum(jnp.where(jnp.arange(prompts) == x, prefix_lengths, 0))
    visit_at = lax.broadcasted_iota(jnp.int32, (half + 1, 16), 0)
    item = lax.broadcasted_iota(jnp.int32, (half + 1, 16), 1)
    step_dir = 1 - 2 * rep
    plane = (z - step_dir * visit_at + n_z) % n_z
    slot = jnp.where(item < n_x, item, item - 6) + jnp.where(visit_at % half == 0, 2 * rep, 0)
    from_x = (x - slot + 2 * n_x) % n_x
    meta = jnp.where(item < n_x, (plane * n_x + from_x) * pre_rows < length, plane < z).astype(jnp.int32)
    meta = jnp.where((item == 6) | (item == 7), from_x * chk_rows, meta)
    meta = jnp.where(item == 8, rep * q_rows, jnp.where(item == 9, (1 - rep) * q_rows, meta))

    def visit(state, parts, index, diag):
        rows = sum(p.shape[0] for p in parts)
        flops = 4 * rows * HEAD_DIM * 3 * pre_cols
        return pl.pallas_call(
            lambda *refs: key_kernel(pre_cols, dec_width, index, diag, *refs),
            name="visit",
            out_shape=state_shape,
            in_specs=[SMEM] + [VMEM] * (len(parts) + 2),
            out_specs=VMEM,
            input_output_aliases={len(parts) + 2: 0},
            compiler_params=params,
            cost_estimate=pl.CostEstimate(flops=flops, bytes_accessed=1 << 20, transcendentals=0),
        )(meta, *parts, q_all, state)

    up = [((i * 2), ((i + 1) % n_z) * 2) for i in range(n_z)]
    down = [((i * 2 + 1), ((i - 1) % n_z) * 2 + 1) for i in range(n_z)]

    def hop(parts):
        moved = []
        for part in parts:
            moved.append(lax.ppermute(part, ("blk", "rep"), up + down))
        return moved

    def one_of_two(pair):
        return jnp.where(rep == 0, pair[0], pair[1])

    travel = hop(chunks)
    state = visit(state, [one_of_two(chunks)], 0, True)
    for s in range(1, half):
        here = travel
        travel = hop(here if s + 1 < half else [one_of_two(here)])
        state = visit(state, here, s, False)
    state = visit(state, travel, half, False)

    theirs = lax.ppermute(state[1], "rep", swap)
    where = (x - jnp.arange(steps, dtype=jnp.int32)) % n_x
    dec_tall = row_dev * n_heads // heads_dev
    ready = pl.pallas_call(
        lambda *refs: finish_kernel(n_heads, steps, *refs),
        name="finish",
        out_shape=jax.ShapeDtypeStruct((n_x, q_rows + dec_tall, width), jnp.bfloat16),
        in_specs=[SMEM] + [VMEM] * 3,
        out_specs=VMEM,
        compiler_params=params,
        cost_estimate=pl.CostEstimate(flops=1 << 28, bytes_accessed=1 << 21, transcendentals=0),
    )(where, state, theirs, spread)

    back = lax.all_to_all(ready, "head", split_axis=0, concat_axis=0, tiled=True)
    prefill_out = back[:, :q_rows]
    mine = back[0, q_rows:]
    for j in range(1, n_x):
        mine = mine + back[j, q_rows:]
    around = [mine] + [lax.ppermute(mine, "head", shift(n_x, -k)) for k in range(1, n_x)]
    decoded = jnp.roll(jnp.stack(around), x, axis=0)
    decode_out = jnp.concatenate(
        [decoded[:, i * row_dev : (i + 1) * row_dev] for i in range(n_x)], axis=2
    )
    return (prefill_out, decode_out)


def solution(mesh):
    placed = (
        P("groups", ("blk", "rep"), "head"),
        P("groups", ("blk", "head"), None),
        P("groups", ("blk", "head"), None),
        P("groups", ("blk", "head"), None),
        P("groups", ("blk", "head"), None),
        P("groups"),
        P("groups", "rep", None),
        P("groups", "rep", None),
        P("groups", "rep", None),
        P(("groups", "rep")),
    )
    return jax.shard_map(
        local,
        mesh=mesh,
        in_specs=placed,
        out_specs=(P("groups", ("blk", "rep"), "head"), P("groups", "rep", None)),
        check_vma=False,
    )
```
